32 devices in a mesh: dp: 32 (over z, y, x, core).
Axes of the slice: x: 2, y: 2, z: 4, core: 2. Of those that a mesh axis runs over, the one named last changes fastest.
Arguments:
- gradients: bfloat16 [32, 48, 4608], P('dp'), may hold values from -144 to 144
- owned_rows: int32 [32], replicated, may hold values from 1 to 3, 48 in all
- master: float32 [96, 4608], P('dp'), may hold values from -0.09375 to 0.09375
- first_moment: float32 [96, 4608], P('dp'), may hold values from -0.03125 to 0.03125
- second_moment: float32 [96, 4608], P('dp'), may hold values from 1.3563368e-06 to 1.3563368e-05
Outputs:
- new_master: float32 [96, 4608], P('dp')
- new_first: float32 [96, 4608], P('dp')
- new_second: float32 [96, 4608], P('dp')
- direction: float32 [96, 4608], P('dp')
- weights: bfloat16 [48, 4608], replicated
The draws below stay inside these ranges and needn't reach their ends.
Inputs may be any that keep to these rules, and one draw needn't show every extreme that they name: `owned_rows`: owners hold consecutive flat rows in owner order; the counts sum to 48 and some owner holds exactly 3.
All inputs are finite; a program needn't handle non-finite values.
Results may differ from the reference program's by a relative error of at most 0.001.
Values may be sent and summed in bfloat16 or wider, within the bound.
A program may use at most 128 MiB of HBM per device.

```python
import math
import jax
import jax.numpy as jnp
import numpy as np
from jax import lax

D = 4608
CAP = 3
STEP = 100
ROWS = 48
N_DP = 32


def draw_gradients(key, part):
    base_key, pair_key = jax.random.split(jax.random.fold_in(key, 17))
    rows = jnp.arange(ROWS, dtype=jnp.float32) / ROWS
    base = jnp.clip(jax.random.normal(base_key, (N_DP, ROWS, D), jnp.float32), -6.0, 6.0)
    scale = 1.0 + 5.0 * rows
    pairing = jax.random.permutation(pair_key, N_DP)
    blocks = jnp.arange(ROWS, dtype=jnp.int32) * N_DP // ROWS
    spike = jnp.where(blocks[None, :] == pairing[:, None], 4.0, 1.0)
    return (base * scale[None, :, None] * spike[:, :, None]).astype(jnp.bfloat16)


def steps_of(rng, shape, shards, least, largest):
    loudness = 1.0
    for position, parts in shards:
        draws = jax.random.uniform(jax.random.fold_in(jax.random.fold_in(rng, 6), position), (parts,), jnp.float32, least / len(shards), largest / len(shards))
        loudness = loudness * jnp.repeat(jnp.exp(draws), shape[position] // parts).reshape((-1,) + (1,) * (len(shape) - 1 - position))
    return loudness


def split_up(count, total, most, lean):
    portions = [(1 << 20) // math.isqrt(rank ** lean) + 1 for rank in range(2, count + 1)]
    rest, counts = total - most - (count - 1), [1] * (count - 1)
    while rest > 0:
        candidates = [i for i in range(count - 1) if counts[i] < most]
        whole, left = sum([portions[i] for i in candidates]), rest
        for i in candidates:
            more = min(most - counts[i], max(1, left * portions[i] // whole), rest)
            counts[i] = counts[i] + more
            rest = rest - more
    return np.array([most] + counts)


def ragged(own_key, amount, total, bound, skew):
    if amount == 2:
        one = jax.random.randint(own_key, (), max(1, total - bound), min(bound, total - 1) + 1)
        return jnp.stack([one, total - one])
    tallies = jnp.asarray(split_up(amount, total, bound, skew), jnp.int32)
    pairs = (amount - 1) // 2
    giver, receiver = tallies[1:1 + 2 * pairs:2], tallies[2:2 + 2 * pairs:2]
    room = jnp.minimum(giver - 1, bound - receiver)
    passed = jax.random.randint(jax.random.fold_in(own_key, 1), (pairs,), 0, 1 << 20) % (room + 1)
    tallies = tallies.at[1:1 + 2 * pairs:2].set(giver - passed).at[2:2 + 2 * pairs:2].set(receiver + passed)
    return tallies[jax.random.permutation(jax.random.fold_in(own_key, 2), amount)]


def bell_draw(key, extent, scale, bound, pieces=(), held_as=jnp.bfloat16):
    values = scale * jax.random.normal(key, extent, jnp.float32)
    if pieces:
        values = values * steps_of(key, extent, pieces, -0.22, 0.18)
    return jnp.clip(values, -bound, bound).astype(held_as)


def setup_inputs(seed: int = 0) -> dict:
    splits = jax.random.split(jax.random.key(seed), 6)
    gradients = draw_gradients(jax.random.fold_in(splits[5], 71), 0)
    owned_rows = ragged(splits[1], N_DP, ROWS, CAP, 2).astype(jnp.int32)
    master = bell_draw(splits[2], (N_DP * CAP, D), D ** -0.5, 0.09375, ((0, 32),), jnp.float32)
    first_moment = bell_draw(splits[3], (N_DP * CAP, D), (1.0 / (ROWS * D) ** 0.5), 0.03125, ((0, 32),), jnp.float32)
    second_moment = jnp.clip(jnp.exp(math.log(1.3563368156610522e-05) - 2.3025851 * jax.random.uniform(splits[4], (N_DP * CAP, D), jnp.float32) ** steps_of(splits[4], (N_DP * CAP, D), ((0, 32),), -0.2, 0.2)), 1.3563368383984198e-06, 1.3563368156610522e-05)
    return {"gradients": gradients, "owned_rows": owned_rows, "master": master, "first_moment": first_moment, "second_moment": second_moment}


beta_one = 0.9
beta_two = 0.999
adam_eps = 1e-08
learn_rate = 0.001
decay_rate = 0.1
clip_norm = 1.0

def slot_layout(owned_rows):
    row_starts = (jnp.cumsum(owned_rows) - owned_rows).astype(jnp.int32)
    slot_list = jnp.arange(N_DP * CAP, dtype=jnp.int32)
    owner_of = slot_list // CAP
    within_slot = slot_list % CAP
    live_mask = within_slot < owned_rows[owner_of]
    flat_rows = jnp.where(live_mask, row_starts[owner_of] + within_slot, 0).astype(jnp.int32)
    return (row_starts, flat_rows, live_mask)

def reference(gradients, owned_rows, master, first_moment, second_moment):

    def accumulate(running, replica_grad):
        return (running + replica_grad.astype(jnp.float32), None)
    summed, _ = lax.scan(accumulate, jnp.zeros((ROWS, D), jnp.float32), gradients)
    norm_sq = jnp.sum(summed * summed)
    clip_scale = jnp.minimum(1.0, clip_norm / (jnp.sqrt(norm_sq) + 1e-06))
    row_starts, flat_rows, live_mask = slot_layout(owned_rows)
    live_rows = live_mask[:, None]
    slot_grad = jnp.where(live_rows, summed[flat_rows], 0.0) * clip_scale
    new_first = beta_one * first_moment + (1.0 - beta_one) * slot_grad
    new_second = beta_two * second_moment + (1.0 - beta_two) * slot_grad * slot_grad
    first_hat = new_first / (1.0 - beta_one ** STEP)
    second_hat = new_second / (1.0 - beta_two ** STEP)
    direction = first_hat / (jnp.sqrt(second_hat) + adam_eps) + decay_rate * master
    new_master = master - learn_rate * direction
    new_master = jnp.where(live_rows, new_master, 0.0)
    new_first = jnp.where(live_rows, new_first, 0.0)
    new_second = jnp.where(live_rows, new_second, 0.0)
    direction = jnp.where(live_rows, direction, 0.0)
    slot_weights = new_master.astype(jnp.bfloat16)
    row_list = jnp.arange(ROWS, dtype=jnp.int32)
    row_owner = (lax.optimization_barrier(jnp.sum((row_starts[None, :] <= row_list[:, None]).astype(jnp.int32), axis=1)) - 1).astype(jnp.int32)
    row_slot = (row_owner * CAP + row_list - row_starts[row_owner]).astype(jnp.int32)
    weights = slot_weights[row_slot]
    return (new_master, new_first, new_second, direction, weights)
```

```python
import functools

import jax
import jax.numpy as jnp
from jax import lax
from jax.experimental import pallas as pl
from jax.experimental.pallas import tpu as pltpu
from jax.sharding import PartitionSpec as P

STEP = 100
beta_one = 0.9
beta_two = 0.999
adam_eps = 1e-08
learn_rate = 0.001
decay_rate = 0.1
clip_norm = 1.0

LANES = 128
SUBLANES = 8
MESH = pl.DeviceIdType.MESH


def adam(slot_grad, master, first, second, live):
    new_first = beta_one * first + (1.0 - beta_one) * slot_grad
    new_second = beta_two * second + (1.0 - beta_two) * slot_grad * slot_grad
    first_hat = new_first * (1.0 / (1.0 - beta_one**STEP))
    second_hat = new_second * (1.0 / (1.0 - beta_two**STEP))
    direction = first_hat / (jnp.sqrt(second_hat) + adam_eps) + decay_rate * master
    new_master = master - learn_rate * direction
    zero = jnp.zeros_like(new_master)
    return tuple(jnp.where(live, v, zero) for v in (new_master, new_first, new_second, direction))


def kernel(cfg, owned_ref, g_hbm, m_hbm, f_hbm, s_hbm,
           grad_hbm, w_hbm,
           g_buf, p0_land, pair, p1_land, p2_land, sel, st, st_land, ship, own_land,
           np_send, np_land, w_send, w_land, c_buf, stage, m_buf, f_buf, s_buf, grad_buf,
           g_sem, in_sem, out_sem, w_sem,
           p0_s, p0_r, p1_s, p1_r, st_s, st_r, p2_s, p2_r, sh_s, sh_r, np_s, np_r, p4_s, p4_r,
           p5_s, p5_r, fw_s, fw_r):
    n, group, lines, rows, cap, tiles, win, base = cfg
    me = lax.axis_index("dp")
    k = me % group
    z = me // group
    width = win * LANES
    slots = cap * group
    small = tiles // group
    head = (win + 1) // 2
    chunks = [(0, head), (head, win - head)] if win > head else [(0, win)]

    def col(j):
        return pl.multiple_of(((j * tiles) // group) * LANES, LANES)

    def at_col(j, first, count):
        return pl.ds(pl.multiple_of(col(j) + first * LANES, LANES), count * LANES)

    def xor(a, b):
        out = a
        bit = 1
        while bit <= b:
            if b & bit:
                out = out + bit - 2 * bit * ((a // bit) % 2)
            bit *= 2
        return out

    def plane(d):
        return z * group + xor(k, d)

    def line(d):
        return xor(z, d) * group + k

    load = pltpu.make_async_copy(g_hbm.at[0], g_buf, g_sem)
    load.start()
    states = [pltpu.make_async_copy(src, dst, in_sem.at[i]) for i, (src, dst) in
              enumerate(((m_hbm, m_buf), (f_hbm, f_buf), (s_hbm, s_buf)))]
    for copy in states:
        copy.start()
    barrier = pltpu.get_barrier_semaphore()
    for d in range(1, group):
        pl.semaphore_signal(barrier, inc=1, device_id=(plane(d),), device_id_type=MESH)
    for d in range(1, lines):
        pl.semaphore_signal(barrier, inc=1, device_id=(line(d),), device_id_type=MESH)
    pl.semaphore_wait(barrier, group - 1 + lines - 1)
    load.wait()

    def remote(src, dst, ssem, rsem, dev):
        return pltpu.make_async_remote_copy(
            src_ref=src, dst_ref=dst, send_sem=ssem, recv_sem=rsem,
            device_id=(dev,), device_id_type=MESH)

    started = []

    def launch(*args):
        copy = remote(*args)
        copy.start()
        started.append(copy)
        return copy

    order = sorted(range(1, group), key=lambda d: -bin(d).count("1"))
    far = list(range(lines - 1, 0, -1))
    chips = [d // 2 for d in order if d % 2 == 0]
    p0 = {}
    for e in chips + [0]:
        p0[e] = launch(g_buf.at[:, at_col(xor(k, 2 * e + 1), 0, win)], p0_land.at[e],
                       p0_s.at[e], p0_r.at[e], plane(1))
    p1 = {}
    for i, (first, count) in enumerate(chunks):
        lanes = pl.ds(first * LANES, count * LANES)
        for e in chips:
            if i == 0:
                p0[e].wait_recv()
            both = (g_buf[:, at_col(xor(k, 2 * e), first, count)].astype(jnp.float32)
                    + p0_land[e, :, lanes].astype(jnp.float32))
            pair[e, :, lanes] = both.astype(jnp.bfloat16)
            p1[i, e] = launch(pair.at[e, :, lanes], p1_land.at[e, :, lanes],
                              p1_s.at[i, e], p1_r.at[i, e], plane(2 * e))
    p0[0].wait_recv()

    for copy in states:
        copy.wait()
    st[...] = jnp.zeros_like(st)
    st[0:cap, :] = m_buf[...]
    st[cap:2 * cap, :] = f_buf[...]
    st[2 * cap:3 * cap, :] = s_buf[...]
    stc = {}
    for d in order:
        stc[d] = launch(st.at[:, at_col(xor(k, d), 0, win)], st_land.at[d],
                        st_s.at[d], st_r.at[d], plane(d))

    total = lines * slots
    q = lax.broadcasted_iota(jnp.int32, (total, n), 0)
    o = lax.broadcasted_iota(jnp.int32, (total, n), 1)
    q_owner = group * (q // slots) + q % group
    owned = jnp.broadcast_to(owned_ref[...], (total, n))
    count_q = jnp.sum(jnp.where(o == q_owner, owned, 0), axis=1, keepdims=True)
    start_q = jnp.sum(jnp.where(o < q_owner, owned, 0), axis=1, keepdims=True)
    q2 = lax.broadcasted_iota(jnp.int32, (total, rows), 0)
    r2 = lax.broadcasted_iota(jnp.int32, (total, rows), 1)
    j2 = (q2 % slots) // group
    hit = (r2 == start_q + j2) & (j2 < count_q)
    one_hot = jnp.where(hit, 1.0, 0.0)
    for i in range(lines):
        sel[i] = one_hot[i * slots:(i + 1) * slots]

    p2 = {}
    for i, (first, count) in enumerate(chunks):
        lanes = pl.ds(first * LANES, count * LANES)
        part = (g_buf[:, at_col(k, first, count)].astype(jnp.float32)
                + p0_land[0, :, lanes].astype(jnp.float32))
        for e in reversed(chips):
            p1[i, e].wait_recv()
            part = part + p1_land[e, :, lanes].astype(jnp.float32)
        p2_land[0, :, lanes] = part.astype(jnp.bfloat16)
        for d in far:
            p2[i, d] = launch(p2_land.at[0, :, lanes], p2_land.at[d, :, lanes],
                              p2_s.at[i, d], p2_r.at[i, d], line(d))

    for d in range(1, group):
        stc[d].wait_recv()
    for d in range(group):
        at = pl.ds(pl.multiple_of(xor(k, d) * base, SUBLANES), base)
        block = st[:, at_col(k, 0, win)] if d == 0 else st_land[d]
        for c in range(win):
            c_buf[c, at, :] = block[:, c * LANES:(c + 1) * LANES]

    own_width = ((k + 1) * tiles) // group - (k * tiles) // group
    norm_tile = jnp.zeros((SUBLANES, LANES), jnp.float32)
    for i, (first, count) in enumerate(chunks):
        lanes = pl.ds(first * LANES, count * LANES)
        whole = p2_land[0, :, lanes].astype(jnp.float32)
        for d in range(1, lines):
            p2[i, d].wait_recv()
            whole = whole + p2_land[d, :, lanes].astype(jnp.float32)
        squares = whole * whole
        for c in range(count):
            tile = squares[0:SUBLANES, c * LANES:(c + 1) * LANES]
            for r in range(1, rows // SUBLANES):
                tile = tile + squares[r * SUBLANES:(r + 1) * SUBLANES, c * LANES:(c + 1) * LANES]
            if first + c >= small:
                inside = jnp.full((SUBLANES, LANES), own_width, jnp.int32) > first + c
                tile = jnp.where(inside, tile, 0.0)
            norm_tile = norm_tile + tile
    np_send[...] = norm_tile
    np_land[k] = norm_tile
    npl = {}
    for d in order:
        npl[d] = launch(np_send, np_land.at[k], np_s.at[d], np_r.at[d], plane(d))

    my_sel = sel[z]
    live = jnp.sum(my_sel, axis=1, keepdims=True) > 0.5
    my_sel = my_sel.astype(jnp.bfloat16)
    summed = jnp.dot(my_sel, p2_land[0], preferred_element_type=jnp.float32)
    for d in range(1, lines):
        summed = summed + jnp.dot(my_sel, p2_land[d], preferred_element_type=jnp.float32)
    for j in range(cap):
        for c in range(win):
            ship[c, pl.ds(j, group, stride=SUBLANES), :] = summed[
                j * group:(j + 1) * group, c * LANES:(c + 1) * LANES]
    sh = {}
    for d in order:
        rows_to = pl.ds(pl.multiple_of(xor(k, d) * SUBLANES, SUBLANES), SUBLANES)
        sh[d] = launch(ship.at[:, rows_to, :], own_land.at[d],
                       sh_s.at[d], sh_r.at[d], plane(d))

    def state(a):
        return jnp.concatenate([
            jnp.concatenate([c_buf[c, pl.ds(a * cap + j, group, stride=base), :]
                             for c in range(win)], axis=1)
            for j in range(cap)], axis=0)

    master_c, first_c, second_c = state(0), state(1), state(2)
    for d in range(1, group):
        npl[d].wait_recv()
    tile = np_land[0]
    for i in range(1, group):
        tile = tile + np_land[i]
    norm_sq = jnp.sum(jnp.sum(tile, axis=0, keepdims=True), axis=1, keepdims=True)
    clip = jnp.minimum(1.0, clip_norm / (jnp.sqrt(norm_sq) + 1e-06))

    w_send[...] = adam(summed * clip, master_c, first_c, second_c, live)[0].astype(jnp.bfloat16)
    p4 = {}
    for i, (first, count) in enumerate(chunks):
        lanes = pl.ds(first * LANES, count * LANES)
        for d in far:
            p4[i, d] = launch(w_send.at[:, lanes], w_land.at[d, :, lanes],
                              p4_s.at[i, d], p4_r.at[i, d], line(d))

    for d in range(1, group):
        sh[d].wait_recv()
    for d in range(group):
        if d == 0:
            pieces = [ship[c, pl.ds(pl.multiple_of(k * SUBLANES, SUBLANES), SUBLANES), :]
                      for c in range(win)]
        else:
            pieces = [own_land[d, c] for c in range(win)]
        g_own = jnp.concatenate(pieces, axis=1)[0:cap]
        grad_buf[:, at_col(xor(k, d), 0, win)] = g_own * clip
    grad_out = pltpu.make_async_copy(grad_buf, grad_hbm, out_sem)
    grad_out.start()

    def spread(i, x):
        return lax.dot_general(sel[i].astype(jnp.bfloat16), x, (((0,), (0,)), ((), ())),
                               preferred_element_type=jnp.float32)

    def wide(j):
        return ((j + 1) * tiles) // group - (j * tiles) // group > small

    def final(src_k, first, count):
        return w_hbm.at[:, at_col(src_k, first, count)]

    local, inward = [], []

    def settle(i, e):
        src_k, from_k = xor(k, 2 * e), xor(k, 2 * e + 1)
        first, count = chunks[i]
        sure = min(count, small - first)
        parts = [(i, first, sure, None)] if sure > 0 else []
        if first + count > small:
            parts.append((2, small, 1, (wide(src_k), wide(from_k))))
        for t, begin, span, when in parts:
            src = stage.at[e, :, pl.ds(begin * LANES, span * LANES)]
            ahead = remote(src, final(src_k, begin, span), fw_s.at[t, e], fw_r.at[t, e], plane(1))
            here = pltpu.make_async_copy(src, final(src_k, begin, span), w_sem.at[t, e])
            if when is None:
                ahead.start()
                here.start()
            else:
                @pl.when(when[0])
                def _(ahead=ahead, here=here):
                    ahead.start()
                    here.start()
            back = remote(src, final(from_k, begin, span), fw_s.at[t, e], fw_r.at[t, e], plane(1))
            local.append((ahead, here, when))
            inward.append((back, when))

    p5 = {}
    for i, (first, count) in enumerate(chunks):
        lanes = pl.ds(first * LANES, count * LANES)
        flat = spread(z, w_send[:, lanes])
        for d in range(1, lines):
            p4[i, d].wait_recv()
            flat = flat + spread(xor(z, d), w_land[d, :, lanes])
        stage[0, :, lanes] = flat.astype(jnp.bfloat16)
        for e in chips:
            p5[i, e] = launch(stage.at[0, :, lanes], stage.at[e, :, lanes],
                              p5_s.at[i, e], p5_r.at[i, e], plane(2 * e))
        settle(i, 0)
    for i in range(len(chunks)):
        for e in reversed(chips):
            p5[i, e].wait_recv()
            settle(i, e)
    grad_out.wait()
    for back, when in inward:
        if when is None:
            back.wait_recv()
        else:
            pl.when(when[1])(back.wait_recv)
    for ahead, here, when in local:
        def done(ahead=ahead, here=here):
            ahead.wait_send()
            here.wait()
        if when is None:
            done()
        else:
            pl.when(when[0])(done)
    for copy in started:
        copy.wait_send()


def finish(owned_ref, g_ref, m_ref, f_ref, s_ref, w_ref,
           nm_ref, nf_ref, ns_ref, dr_ref, out_ref):
    out_ref[...] = w_ref[...]
    me = lax.axis_index("dp")
    cap = m_ref.shape[0]
    o = lax.broadcasted_iota(jnp.int32, owned_ref.shape, 1)
    count = jnp.sum(jnp.where(o == me, owned_ref[...], 0), axis=1, keepdims=True)
    live = lax.broadcasted_iota(jnp.int32, m_ref.shape, 0) < count
    outs = adam(g_ref[...], m_ref[...], f_ref[...], s_ref[...], live)
    for ref, v in zip((nm_ref, nf_ref, ns_ref, dr_ref), outs):
        ref[...] = v


def per_device(n, gradients, owned_rows, master, first_moment, second_moment):
    rows, width_all = gradients.shape[1:]
    cap = master.shape[0]
    group = 16
    while n % group:
        group //= 2
    lines = n // group
    tiles = width_all // LANES
    win = -(-tiles // group)
    width = win * LANES
    slots = cap * group
    base = -(-3 * cap // SUBLANES) * SUBLANES
    cfg = (n, group, lines, rows, cap, tiles, win, base)
    f32, b16 = jnp.float32, jnp.bfloat16
    sds = jax.ShapeDtypeStruct((cap, width_all), f32)
    weights_type = jax.ShapeDtypeStruct((rows, width_all), b16)
    vm = pl.BlockSpec(memory_space=pltpu.VMEM)
    anym = pl.BlockSpec(memory_space=pl.ANY)
    dma = pltpu.SemaphoreType.DMA
    scratch = [
        pltpu.VMEM((rows, width_all), b16),
        pltpu.VMEM((group // 2, rows, width), b16),
        pltpu.VMEM((group // 2, rows, width), b16),
        pltpu.VMEM((group // 2, rows, width), b16),
        pltpu.VMEM((lines, rows, width), b16),
        pltpu.VMEM((lines, slots, rows), f32),
        pltpu.VMEM((base, width_all), f32),
        pltpu.VMEM((group, base, width), f32),
        pltpu.VMEM((win, group * SUBLANES, LANES), f32),
        pltpu.VMEM((group, win, SUBLANES, LANES), f32),
        pltpu.VMEM((SUBLANES, LANES), f32),
        pltpu.VMEM((group, SUBLANES, LANES), f32),
        pltpu.VMEM((slots, width), b16),
        pltpu.VMEM((lines, slots, width), b16),
        pltpu.VMEM((win, group * base, LANES), f32),
        pltpu.VMEM((group // 2, rows, width), b16),
        pltpu.VMEM((cap, width_all), f32),
        pltpu.VMEM((cap, width_all), f32),
        pltpu.VMEM((cap, width_all), f32),
        pltpu.VMEM((cap, width_all), f32),
        dma, dma((3,)), dma, dma((3, group // 2)),
        dma((group // 2,)), dma((group // 2,)),
        dma((2, group // 2)), dma((2, group // 2)), dma((group,)), dma((group,)),
        dma((2, lines)), dma((2, lines)), dma((group,)), dma((group,)),
        dma((group,)), dma((group,)), dma((2, lines)), dma((2, lines)),
        dma((2, group // 2)), dma((2, group // 2)), dma((3, group // 2)), dma((3, group // 2)),
    ]
    owned = owned_rows.reshape(1, n)
    slot_grad, gathered = pl.pallas_call(
        functools.partial(kernel, cfg),
        out_shape=(sds, weights_type),
        in_specs=[vm, anym, anym, anym, anym],
        out_specs=(anym, anym),
        scratch_shapes=scratch,
        compiler_params=pltpu.CompilerParams(collective_id=0, has_side_effects=True),
    )(owned, gradients, master, first_moment, second_moment)
    return pl.pallas_call(
        finish,
        out_shape=(sds, sds, sds, sds, weights_type),
        in_specs=[vm] * 6,
        out_specs=(vm,) * 5,
    )(owned, slot_grad, master, first_moment, second_moment, gathered)


def solution(mesh):
    in_specs = (P("dp", None, None), P(), P("dp", None), P("dp", None), P("dp", None))
    out_specs = (P("dp", None), P("dp", None), P("dp", None), P("dp", None), P())
    return jax.shard_map(
        functools.partial(per_device, mesh.shape["dp"]),
        mesh=mesh, in_specs=in_specs, out_specs=out_specs, check_vma=False
    )
```

```python
import functools

import jax
import jax.numpy as jnp
from jax import lax
from jax.experimental import pallas as pl
from jax.experimental.pallas import tpu as pltpu
from jax.sharding import PartitionSpec as P

STEP = 100
beta_one = 0.9
beta_two = 0.999
adam_eps = 1e-08
learn_rate = 0.001
decay_rate = 0.1
clip_norm = 1.0

LANES = 128
SUBLANES = 8
PACK = 16
VMEM_BYTES = 67043328
MESH = pl.DeviceIdType.MESH


def adam(slot_grad, master, first, second):
    new_first = beta_one * first + (1.0 - beta_one) * slot_grad
    new_second = beta_two * second + (1.0 - beta_two) * slot_grad * slot_grad
    first_hat = new_first * (1.0 / (1.0 - beta_one**STEP))
    second_hat = new_second * (1.0 / (1.0 - beta_two**STEP))
    direction = first_hat / (jnp.sqrt(second_hat) + adam_eps) + decay_rate * master
    new_master = master - learn_rate * direction
    return new_master, new_first, new_second, direction


def xor(a, b, top):
    out = 0
    bit = 1
    while bit < top:
        out = out + bit * (((a // bit) + (b // bit)) % 2)
        bit *= 2
    return out


def extra_table(group, extra):
    even = [t for t in range(group // 2) if bin(t).count("1") % 2 == 0]
    half = extra // 2
    assert extra % 2 == 0 and extra <= len(even)
    return [[even[core * half + i] for i in range(half)] for core in range(2)]


def kernel(cfg, owned_hbm, g_hbm, m_hbm, f_hbm, s_hbm,
           nm_ref, nf_ref, ns_ref, dr_ref, w_ref,
           owned_v, grad_ref, g_buf, m_buf, f_buf, s_buf, st32, st, st_all, flat,
           p0_land, pair, p1_land, h, p0x_land, pairx, p1x_land, hx,
           np_send, np_land, ship, own_land, shipx, own_landx,
           own_sem, g_sem, in_sem,
           p0_s, p0_r, p0x_s, p0x_r, p1_s, p1_r, p1x_s, p1x_r,
           h_s, h_r, hx_s, hx_r, ln_s, ln_r, st_s, st_r, stx_s, stx_r,
           np_s, np_r, sh_s, sh_r, shx_s, shx_r,
           ag_s, ag_r, agx_s, agx_r, fw_s, fw_r, fwx_s, fwx_r):
    n, group, lines, rows, cap, tiles, main, extra = cfg
    half = extra // 2
    table = extra_table(group, extra)
    base = group * main
    f32, b16 = jnp.float32, jnp.bfloat16
    me = lax.axis_index("dp")
    k = me % group
    z = me // group
    chip = k // 2
    core = k % 2
    nchips = group // 2
    slots = cap * group
    mw = main * LANES

    def main_at(j):
        return pl.ds(pl.multiple_of(j * mw, LANES), mw)

    def tile_at(t, count=1):
        return pl.ds(pl.multiple_of(t * LANES, LANES), count * LANES)

    def plane(d):
        return z * group + xor(k, d, group)

    def line(d):
        return xor(z, d, lines) * group + k

    def holder(c, i):
        return table[0][i] + c * (table[1][i] - table[0][i])

    mine = [chip == holder(core, i) for i in range(half)]
    i_me = 0
    wide = False
    for i in range(half):
        i_me = i_me + i * jnp.where(mine[i], 1, 0)
        wide = jnp.logical_or(wide, mine[i])

    owned_cp = pltpu.make_async_copy(owned_hbm, owned_v, own_sem)
    load = pltpu.make_async_copy(g_hbm.at[0], g_buf, g_sem)
    load.start()
    states = [pltpu.make_async_copy(src, dst, in_sem.at[i]) for i, (src, dst) in
              enumerate(((m_hbm, m_buf), (f_hbm, f_buf), (s_hbm, s_buf)))]
    for copy in states:
        copy.start()
    owned_cp.start()
    barrier = pltpu.get_barrier_semaphore()
    for d in range(1, group):
        pl.semaphore_signal(barrier, inc=1, device_id=(plane(d),), device_id_type=MESH)
    for d in range(1, lines):
        pl.semaphore_signal(barrier, inc=1, device_id=(line(d),), device_id_type=MESH)
    pl.semaphore_wait(barrier, group - 1 + lines - 1)
    load.wait()

    def remote(src, dst, ssem, rsem, dev):
        return pltpu.make_async_remote_copy(
            src_ref=src, dst_ref=dst, send_sem=ssem, recv_sem=rsem,
            device_id=(dev,), device_id_type=MESH)

    started = []

    def launch(*args, when=None):
        copy = remote(*args)
        if when is None:
            copy.start()
        else:
            pl.when(when)(copy.start)
        started.append((copy, when))
        return copy

    def on(when, action):
        if when is None:
            action()
        else:
            pl.when(when)(action)

    far = sorted(range(1, nchips), key=lambda e: -bin(e).count("1"))
    peers = sorted(range(1, group), key=lambda d: -bin(d).count("1"))

    p0 = {}
    p0x = launch(g_buf.at[:, tile_at(base + (1 - core) * half, half)], p0x_land, p0x_s, p0x_r, plane(1))
    for e in far + [0]:
        j = 2 * xor(chip, e, nchips) + 1 - core
        p0[e] = launch(g_buf.at[:, main_at(j)], p0_land.at[e], p0_s.at[e], p0_r.at[e], plane(1))

    for copy in states:
        copy.wait()
    owned_cp.wait()

    def split(x):
        high = x.astype(b16).astype(f32)
        return high, x - high

    mh, ml = split(m_buf[...])
    fh, fl = split(f_buf[...])
    st32[...] = jnp.zeros_like(st32)
    for i, part in enumerate((mh, ml, fh, fl, s_buf[...])):
        st32[i * cap:(i + 1) * cap, :] = part
    st[0] = st32[...].astype(b16)

    p0x.wait_recv()
    pairx[...] = (g_buf[:, tile_at(base + core * half, half)].astype(f32) + p0x_land[...].astype(f32)).astype(b16)
    for i in range(half):
        t = holder(core, i)
        dist = xor(chip, t, nchips)
        launch(pairx.at[:, i * LANES:(i + 1) * LANES], p1x_land.at[dist], p1x_s.at[i], p1x_r.at[dist],
               z * group + 2 * t + core, when=jnp.logical_not(mine[i]))
    p1 = {}
    for e in far:
        p0[e].wait_recv()
        j = 2 * xor(chip, e, nchips) + core
        pair[e] = (g_buf[:, main_at(j)].astype(f32) + p0_land[e].astype(f32)).astype(b16)
        p1[e] = launch(pair.at[e], p1_land.at[e], p1_s.at[e], p1_r.at[e], plane(2 * e))

    ln = {}
    for d in range(1, lines):
        ln[d] = launch(st.at[0], st.at[d], ln_s.at[d], ln_r.at[d], line(d))

    stw = {}
    stx_when = [jnp.logical_not(jnp.logical_and(chip == table[e // half][e % half], core == e // half))
                for e in range(extra)]

    def spread_state(l):
        for d in peers:
            at = pl.ds((l * group + d) * PACK, PACK)
            stw[l, d] = launch(st.at[l, :, main_at(xor(k, d, group))], st_all.at[at, 0:mw],
                               st_s.at[l, d], st_r.at[l, d], plane(d))
        for e in range(extra):
            j = 2 * table[e // half][e % half] + e // half
            dist = xor(k, j, group)
            at = pl.ds(pl.multiple_of((l * group + dist) * PACK, PACK), PACK)
            launch(st.at[l, :, tile_at(base + e)], st_all.at[at, mw:mw + LANES],
                   stx_s.at[l, e], stx_r.at[l, dist], z * group + j, when=stx_when[e])

    spread_state(0)

    unit = group * PACK
    q = lax.broadcasted_iota(jnp.int32, (1, unit), 1)
    part_q = q % PACK
    slot_q = part_q % cap
    kind_q = part_q // cap
    number = lax.broadcasted_iota(jnp.int32, (n, unit), 0)
    square = (n, n)
    diagonal = lax.broadcasted_iota(jnp.int32, square, 0) == lax.broadcasted_iota(jnp.int32, square, 1)
    column = jnp.sum(jnp.where(diagonal, jnp.broadcast_to(owned_v[...], square), 0), axis=1, keepdims=True)
    owned = jnp.broadcast_to(column, (n, unit))
    row = lax.broadcasted_iota(jnp.int32, (rows, unit), 0)

    def row_of(owner, slot):
        shape = owned.shape
        owner = jnp.broadcast_to(owner, shape)
        count = jnp.sum(jnp.where(number == owner, owned, 0), axis=0, keepdims=True)
        start = jnp.sum(jnp.where(number < owner, owned, 0), axis=0, keepdims=True)
        return jnp.where(slot < count, start + slot, -1)

    def picks(l):
        owner = xor(l, z, lines) * group + ((q // PACK) ^ k)
        at = jnp.where(kind_q < 5, row_of(owner, slot_q), -1)
        hit = row == jnp.broadcast_to(at, row.shape)
        kind = jnp.broadcast_to(kind_q // 2, row.shape)
        return jnp.concatenate(
            [jnp.where(jnp.logical_and(hit, kind == i), 1.0, 0.0) for i in range(3)], axis=0).astype(b16)

    q2 = lax.broadcasted_iota(jnp.int32, (1, unit), 1)
    at2 = jnp.where(q2 < slots, row_of(z * group + ((q2 % group) ^ k), q2 // group), -1)
    sel = jnp.where(row == jnp.broadcast_to(at2, row.shape), 1.0, 0.0)[:, 0:slots].astype(b16)

    part = g_buf[:, main_at(k)].astype(f32)
    p0[0].wait_recv()
    part = part + p0_land[0].astype(f32)
    for e in reversed(far):
        p1[e].wait_recv()
        part = part + p1_land[e].astype(f32)
    h[0] = part.astype(b16)
    hc = {}
    for d in range(1, lines):
        hc[d] = launch(h.at[0], h.at[d], h_s.at[d], h_r.at[d], line(d))

    @pl.when(wide)
    def _():
        total = pairx[:, tile_at(i_me)].astype(f32)
        for e in reversed(far):
            remote(pairx.at[:, 0:LANES], p1x_land.at[e], p1x_s.at[0], p1x_r.at[e], plane(2 * e)).wait_recv()
            total = total + p1x_land[e].astype(f32)
        hx[0] = total.astype(b16)

    hxc = {}
    for d in range(1, lines):
        hxc[d] = launch(hx.at[0], hx.at[d], hx_s.at[d], hx_r.at[d], line(d), when=wide)

    for d in range(1, lines):
        ln[d].wait_recv()
        spread_state(d)

    def merged(ref):
        total = ref[xor(z, 0, lines)].astype(f32)
        for l in range(1, lines):
            total = total + ref[xor(z, l, lines)].astype(f32)
        return total

    def norm_part(x):
        squares = x * x
        tile = jnp.zeros((SUBLANES, LANES), f32)
        for c in range(x.shape[1] // LANES):
            for r in range(rows // SUBLANES):
                tile = tile + squares[r * SUBLANES:(r + 1) * SUBLANES, c * LANES:(c + 1) * LANES]
        return tile

    for d in range(1, lines):
        hc[d].wait_recv()
    summed = merged(h)
    np_send[...] = norm_part(summed)

    @pl.when(wide)
    def _():
        for d in range(1, lines):
            hxc[d].wait_recv()
        np_send[...] = np_send[...] + norm_part(merged(hx))

    np_land[k] = np_send[...]
    npl = {}
    for d in peers:
        npl[d] = launch(np_send, np_land.at[k], np_s.at[d], np_r.at[d], plane(d))

    def slots_of(ref):
        def one(l):
            return lax.dot_general(sel, ref[xor(z, l, lines)], (((0,), (0,)), ((), ())),
                                   preferred_element_type=f32)
        total = one(0)
        for l in range(1, lines):
            total = total + one(l)
        return total

    picked = slots_of(h)
    block = own_land.shape[1]
    for j in range(cap):
        for c in range(main):
            ship[pl.ds(c * cap + j, group, stride=block), :] = picked[
                j * group:(j + 1) * group, c * LANES:(c + 1) * LANES]
    sh = {}
    for d in peers:
        sh[d] = launch(ship.at[pl.ds(d * block, block), :], own_land.at[d], sh_s.at[d], sh_r.at[d], plane(d))

    @pl.when(wide)
    def _():
        pickedx = slots_of(hx)
        for j in range(cap):
            shipx[pl.ds(j, group, stride=SUBLANES), :] = pickedx[j * group:(j + 1) * group, :]
        own_landx[core * half + i_me] = shipx[0:SUBLANES, :]

    for d in peers:
        launch(shipx.at[pl.ds(d * SUBLANES, SUBLANES), :], own_landx.at[core * half + i_me],
               shx_s.at[d], shx_r.at[core * half + i_me], plane(d), when=wide)

    for l in range(lines):
        for d in range(1, group):
            stw[l, d].wait_recv()
        st_all[pl.ds(l * group * PACK, PACK), 0:mw] = st[l, :, main_at(k)]

        @pl.when(wide)
        def _(l=l):
            for d in range(1, group):
                at = pl.ds((l * group + d) * PACK, PACK)
                remote(st.at[l, :, 0:LANES], st_all.at[at, mw:mw + LANES],
                       stx_s.at[l, 0], stx_r.at[l, d], plane(d)).wait_recv()
            st_all[pl.ds(l * group * PACK, PACK), mw:mw + LANES] = st[l, :, tile_at(base + core * half + i_me)]

    def bring(l, total):
        at = pl.ds(pl.multiple_of(l * unit, unit), unit)
        return total + jnp.dot(picks(l), st_all[at, :], preferred_element_type=f32)

    zero = jnp.zeros((3 * rows, mw + LANES), f32)
    if lines <= 2:
        total = zero
        for l in range(lines):
            total = bring(l, total)
        flat[...] = total
    else:
        flat[...] = zero

        def step(l, carry):
            flat[...] = bring(l, flat[...])
            return carry
        lax.fori_loop(0, lines, step, 0)

    for d in range(1, group):
        npl[d].wait_recv()
    tile = np_land[0]
    for i in range(1, group):
        tile = tile + np_land[i]
    norm_sq = jnp.sum(jnp.sum(tile, axis=0, keepdims=True), axis=1, keepdims=True)
    clip = jnp.minimum(1.0, clip_norm / (jnp.sqrt(norm_sq) + 1e-06))

    def updated(x, lanes):
        return adam(x * clip, flat[0:rows, lanes], flat[rows:2 * rows, lanes],
                    flat[2 * rows:3 * rows, lanes])[0].astype(b16)

    w_ref[:, main_at(k)] = updated(merged(h), slice(0, mw))
    ag, fw = {}, {}
    for e in far:
        ag[e] = launch(w_ref.at[:, main_at(k)], w_ref.at[:, main_at(k)], ag_s.at[e], ag_r.at[e], plane(2 * e))
    fw[0] = launch(w_ref.at[:, main_at(k)], w_ref.at[:, main_at(k)], fw_s.at[0], fw_r.at[0], plane(1))

    own_tile = tile_at(base + core * half + i_me)

    @pl.when(wide)
    def _():
        w_ref[:, own_tile] = updated(merged(hx), slice(mw, mw + LANES))

    for e in far:
        launch(w_ref.at[:, own_tile], w_ref.at[:, own_tile], agx_s.at[e], agx_r.at[i_me], plane(2 * e), when=wide)

    for d in range(group):
        if d == 0:
            got = ship[0:block, :]
        else:
            sh[d].wait_recv()
            got = own_land[d]
        piece = jnp.concatenate([got[c * cap:(c + 1) * cap] for c in range(main)], axis=1)
        grad_ref[:, main_at(xor(k, d, group))] = piece * clip
    for e in range(extra):
        j = 2 * table[e // half][e % half] + e // half

        @pl.when(stx_when[e])
        def _(e=e):
            remote(shipx.at[0:SUBLANES, :], own_landx.at[e], shx_s.at[1], shx_r.at[e], plane(1)).wait_recv()
        grad_ref[:, (base + e) * LANES:(base + e + 1) * LANES] = own_landx[e, 0:cap, :] * clip

    own_row = lax.broadcasted_iota(jnp.int32, (1, n), 1)
    count = jnp.sum(jnp.where(own_row == me, owned_v[...], 0), axis=1, keepdims=True)
    live = lax.broadcasted_iota(jnp.int32, m_buf.shape, 0) < count
    outs = adam(grad_ref[...], m_buf[...], f_buf[...], s_buf[...])
    for ref, v in zip((nm_ref, nf_ref, ns_ref, dr_ref), outs):
        ref[...] = jnp.where(live, v, jnp.zeros_like(v))

    def forward_main(e):
        at = main_at(2 * xor(chip, e, nchips) + core)
        if e:
            remote(w_ref.at[:, at], w_ref.at[:, at], ag_s.at[e], ag_r.at[e], plane(2 * e)).wait_recv()
            fw[e] = launch(w_ref.at[:, at], w_ref.at[:, at], fw_s.at[e], fw_r.at[e], plane(1))

    for e in reversed(far):
        forward_main(e)
    for i in range(half):
        at = tile_at(base + core * half + i)

        @pl.when(jnp.logical_not(mine[i]))
        def _(i=i, at=at):
            remote(w_ref.at[:, at], w_ref.at[:, at], agx_s.at[1], agx_r.at[i], plane(2)).wait_recv()
        launch(w_ref.at[:, at], w_ref.at[:, at], fwx_s.at[i], fwx_r.at[i], plane(1))

    for e in [0] + far[::-1]:
        at = main_at(2 * xor(chip, e, nchips) + 1 - core)
        remote(w_ref.at[:, at], w_ref.at[:, at], fw_s.at[e], fw_r.at[e], plane(1)).wait_recv()
    for i in range(half):
        at = tile_at(base + (1 - core) * half + i)
        remote(w_ref.at[:, at], w_ref.at[:, at], fwx_s.at[i], fwx_r.at[i], plane(1)).wait_recv()
    for copy, when in started:
        on(when, copy.wait_send)


def finish(*refs):
    count = (len(refs) - 1) // 2
    sem = refs[-1]
    copies = [pltpu.make_async_copy(refs[i], refs[count + i], sem.at[i]) for i in range(count)]
    for copy in copies:
        copy.start()
    for copy in copies:
        copy.wait()


def per_device(n, gradients, owned_rows, master, first_moment, second_moment):
    rows, width_all = gradients.shape[1:]
    cap = master.shape[0]
    group = 16
    while n % group:
        group //= 2
    lines = n // group
    tiles = width_all // LANES
    main = tiles // group
    extra = tiles - main * group
    cfg = (n, group, lines, rows, cap, tiles, main, extra)
    half = extra // 2
    chips = group // 2
    mw = main * LANES
    block = -(-cap * main // SUBLANES) * SUBLANES
    f32, b16 = jnp.float32, jnp.bfloat16
    sds = jax.ShapeDtypeStruct((cap, width_all), f32)
    weights_type = jax.ShapeDtypeStruct((rows, width_all), b16)
    vm = pl.BlockSpec(memory_space=pltpu.VMEM)
    dma = pltpu.SemaphoreType.DMA
    scratch = [
        pltpu.VMEM((1, n), jnp.int32),
        pltpu.VMEM((cap, width_all), f32),
        pltpu.VMEM((rows, width_all), b16),
        pltpu.VMEM((cap, width_all), f32),
        pltpu.VMEM((cap, width_all), f32),
        pltpu.VMEM((cap, width_all), f32),
        pltpu.VMEM((PACK, width_all), f32),
        pltpu.VMEM((lines, PACK, width_all), b16),
        pltpu.VMEM((lines * group * PACK, mw + LANES), b16),
        pltpu.VMEM((3 * rows, mw + LANES), f32),
        pltpu.VMEM((chips, rows, mw), b16),
        pltpu.VMEM((chips, rows, mw), b16),
        pltpu.VMEM((chips, rows, mw), b16),
        pltpu.VMEM((lines, rows, mw), b16),
        pltpu.VMEM((rows, half * LANES), b16),
        pltpu.VMEM((rows, half * LANES), b16),
        pltpu.VMEM((chips, rows, LANES), b16),
        pltpu.VMEM((lines, rows, LANES), b16),
        pltpu.VMEM((SUBLANES, LANES), f32),
        pltpu.VMEM((group, SUBLANES, LANES), f32),
        pltpu.VMEM((group * block, LANES), f32),
        pltpu.VMEM((group, block, LANES), f32),
        pltpu.VMEM((group * SUBLANES, LANES), f32),
        pltpu.VMEM((extra, SUBLANES, LANES), f32),
        dma, dma, dma((3,)),
        dma((chips,)), dma((chips,)), dma, dma, dma((chips,)), dma((chips,)), dma((half,)), dma((chips,)),
        dma((lines,)), dma((lines,)), dma((lines,)), dma((lines,)), dma((lines,)), dma((lines,)),
        dma((lines, group)), dma((lines, group)), dma((lines, extra)), dma((lines, group)),
        dma((group,)), dma((group,)), dma((group,)), dma((group,)), dma((group,)), dma((extra,)),
        dma((chips,)), dma((chips,)), dma((chips,)), dma((half,)),
        dma((chips,)), dma((chips,)), dma((half,)), dma((half,)),
    ]
    owned = owned_rows.reshape(1, n)
    room = VMEM_BYTES - rows * width_all * 2 - 16 * width_all * 4 - (32 << 10)
    hbm = pl.BlockSpec(memory_space=pltpu.HBM)
    outs = (sds,) * 4 + (weights_type,)
    made = pl.pallas_call(
        functools.partial(kernel, cfg),
        out_shape=tuple(pltpu.VMEM(o.shape, o.dtype) for o in outs),
        in_specs=[hbm] * 5,
        out_specs=(vm,) * 5,
        scratch_shapes=scratch,
        compiler_params=pltpu.CompilerParams(collective_id=0, has_side_effects=True, vmem_limit_bytes=room),
    )(owned, gradients, master, first_moment, second_moment)
    return pl.pallas_call(
        finish,
        out_shape=outs,
        in_specs=[vm] * 5,
        out_specs=(hbm,) * 5,
        scratch_shapes=[dma((5,))],
        compiler_params=pltpu.CompilerParams(vmem_limit_bytes=4 << 20),
    )(*made)


def solution(mesh):
    in_specs = (P("dp", None, None), P(), P("dp", None), P("dp", None), P("dp", None))
    out_specs = (P("dp", None), P("dp", None), P("dp", None), P("dp", None), P())
    return jax.shard_map(
        functools.partial(per_device, mesh.shape["dp"]),
        mesh=mesh, in_specs=in_specs, out_specs=out_specs, check_vma=False
    )
```
